16 devices in a mesh: tp: 2 (over z), dp: 8 (over y, x, core).
Axes of the slice: x: 2, y: 2, z: 2, core: 2. Of those that a mesh axis runs over, the one named last changes fastest.
Arguments:
- design: float32 [131072, 1024], P('dp', 'tp')
- target: float32 [131072], P('dp')
- ridge: float32 [], replicated
Outputs:
- output 1: float32 [1024], replicated
- output 2: float32 [131072], P('dp')
All inputs are finite; a program needn't handle non-finite values.
Results may differ from the reference program's by a relative error of at most 0.001.
Values sent between devices are 32-bit elements.
A program may use at most 1 GiB of HBM per device.

```python
import jax
import jax.numpy as jnp
from jax import lax

FEATURES = 1024
ROWS_DEV = 16384
GROUPS = 8
LOW_RANK = 128

TOTAL_ROWS = ROWS_DEV * GROUPS
HIGHEST = lax.Precision.HIGHEST
CONTRACT_ROWS = (((0,), (0,)), ((), ()))


def setup_inputs(seed: int = 0) -> dict:
    keys = jax.random.split(jax.random.key(seed), 9)
    col_scale = jnp.exp(jax.random.uniform(keys[0], (FEATURES,), jnp.float32, -3.0, 0.0))
    base = jax.random.normal(keys[1], (TOTAL_ROWS, FEATURES), jnp.float32)
    factors = jax.random.normal(keys[2], (TOTAL_ROWS, LOW_RANK), jnp.float32)
    mixing = jax.random.normal(keys[3], (FEATURES, LOW_RANK), jnp.float32) * (0.5 * LOW_RANK ** -0.5)
    shard_gain = jnp.exp(jax.random.uniform(keys[4], (GROUPS, 1), jnp.float32, -1.0, 1.0))
    row_jitter = jnp.exp(jax.random.uniform(keys[5], (GROUPS, ROWS_DEV), jnp.float32, -0.25, 0.25))
    row_gain = (shard_gain * row_jitter).reshape(TOTAL_ROWS, 1)
    mixed = jnp.dot(factors, mixing.T, precision=HIGHEST)
    design = (base * col_scale + mixed) * (row_gain * FEATURES ** -0.5)
    x_true = jax.random.normal(keys[6], (FEATURES,), jnp.float32)
    noise = 0.3 * jax.random.normal(keys[7], (TOTAL_ROWS,), jnp.float32) * row_gain[:, 0]
    target = jnp.dot(design, x_true, precision=HIGHEST) + noise
    diag_mean = jnp.sum(design * design) / FEATURES
    ridge = diag_mean * jax.random.uniform(keys[8], (), jnp.float32, 0.01, 0.04)
    return {'design': design, 'target': target, 'ridge': ridge}


def reference(design, target, ridge):
    gram_mat = lax.dot_general(design, design, CONTRACT_ROWS, precision=HIGHEST, preferred_element_type=jnp.float32)
    moment_vec = lax.dot_general(design, target, CONTRACT_ROWS, precision=HIGHEST, preferred_element_type=jnp.float32)
    chol_low = jnp.linalg.cholesky(gram_mat + ridge * jnp.eye(FEATURES, dtype=jnp.float32))
    half_solve = lax.linalg.triangular_solve(chol_low, moment_vec[:, None], left_side=True, lower=True)
    coeffs = lax.linalg.triangular_solve(chol_low, half_solve, left_side=True, lower=True, transpose_a=True)[:, 0]
    residual = target - jnp.dot(design, coeffs, precision=HIGHEST, preferred_element_type=jnp.float32)
    return coeffs, residual
```

```python
import functools

import jax
import jax.numpy as jnp
from jax import lax
from jax.experimental import pallas as pl
from jax.experimental.pallas import tpu as pltpu
from jax.sharding import PartitionSpec as P

MESH = pl.DeviceIdType.MESH
HIGHEST = lax.Precision.HIGHEST
F32 = jnp.float32
CH = 128
GROUPS = 8
SLOTS = 3


def dot(a, b, ca, cb):
    return lax.dot_general(a, b, (((ca,), (cb,)), ((), ())), precision=HIGHEST, preferred_element_type=F32)


def iota(shape, dim):
    return lax.broadcasted_iota(jnp.int32, shape, dim)


def chol_inverse(s_ref, w_ref):
    w_ref[...] = jnp.where(iota((CH, CH), 0) == iota((CH, CH), 1), 1.0, 0.0).astype(F32)
    lane, sub = iota((8, CH), 1), iota((8, CH), 0)

    def group(g, carry):
        r0 = pl.multiple_of(g * 8, 8)
        rows = s_ref[pl.ds(r0, 8), :]
        inv = w_ref[pl.ds(r0, 8), :]
        cols = [
            jnp.broadcast_to(jnp.sum(jnp.where(lane == r0 + i, rows, 0.0), axis=1, keepdims=True), (8, CH))
            for i in range(8)
        ]
        for i in range(8):
            piv = jnp.broadcast_to(cols[i][i : i + 1, :], (8, CH))
            scale = lax.rsqrt(piv)
            scale = scale * (1.5 - 0.5 * piv * scale * scale)
            coef = jnp.where(sub > i, cols[i] * scale, 0.0)
            u = jnp.broadcast_to(rows[i : i + 1, :], (8, CH)) * scale
            v = jnp.broadcast_to(inv[i : i + 1, :], (8, CH)) * scale
            rows = jnp.where(sub == i, u, rows - coef * u)
            inv = jnp.where(sub == i, v, inv - coef * v)
            for j in range(i + 1, 8):
                cols[j] = cols[j] - coef * jnp.broadcast_to(coef[j : j + 1, :], (8, CH))
        w_ref[pl.ds(r0, 8), :] = inv
        below = jnp.where(lane >= r0 + 8, rows, 0.0)
        upd = dot(below, jnp.concatenate([rows, inv], axis=1), 0, 0)
        s_ref[...] -= upd[:, :CH]
        w_ref[...] -= upd[:, CH:]
        return carry

    lax.fori_loop(0, CH // 8, group, 0)


def kernel(
    lam_ref, b_ref, a_hbm, x_ref, r_ref,
    a_v, xr, gacc, hacc, drecv, hrecv, gall, hall, cacc, crecv, cg, pan, lp, linv, s0, s1, w0, w1, nbuf, hpos, ybuf, pbuf, prec,
    load_sem, xs_sem, xr_sem, ds_sem, dr_sem, hs_sem, hr_sem, gs_sem, gr_sem, rs_sem, rr_sem, ps_sem, pr_sem,
):
    rows, cols = a_v.shape
    half = rows // 2
    nch = cols // CH
    subs = xr_sem.shape[1]
    srows = half // subs
    nload = load_sem.shape[0]
    lrows = rows // nload
    t = lax.axis_index("tp")
    d = lax.axis_index("dp")
    other = 1 - t

    def peer(off):
        return lax.rem(d + off, GROUPS)

    def remote(src, dst, ssem, rsem, tp, dp):
        return pltpu.make_async_remote_copy(
            src_ref=src, dst_ref=dst, send_sem=ssem, recv_sem=rsem, device_id={"tp": tp, "dp": dp}, device_id_type=MESH
        )

    def load(i):
        sl = pl.ds(pl.multiple_of(i * lrows, lrows), lrows)
        return pltpu.make_async_copy(a_hbm.at[sl, :], a_v.at[sl, :], load_sem.at[i])

    barrier = pltpu.get_barrier_semaphore()
    pl.semaphore_signal(barrier, inc=1, device_id={"tp": other, "dp": d}, device_id_type=MESH)
    for off in range(1, GROUPS):
        pl.semaphore_signal(barrier, inc=1, device_id={"tp": t, "dp": peer(off)}, device_id_type=MESH)
    for i in range(nload):
        load(i).start()
    pl.semaphore_wait(barrier, GROUPS)

    def exchange(q):
        c, s = q // subs, q % subs
        src = a_hbm.at[pl.ds(pl.multiple_of(other * half + s * srows, srows), srows), pl.ds(c * CH, CH)]
        return remote(src, xr.at[c % SLOTS, pl.ds(s * srows, srows), :], xs_sem.at[c, s], xr_sem.at[c, s], other, d)

    def issue(lo, hi):
        for q in range(lo, hi):
            exchange(q).start()

    total = nch * subs
    ahead = [subs + 3] + [min((k + 2) * subs + 2, total) for k in range(nch)]
    issue(0, ahead[0])

    gacc[...] = jnp.zeros_like(gacc)
    hacc[...] = jnp.zeros_like(hacc)
    pan[...] = jnp.zeros_like(pan)
    lp[...] = jnp.zeros_like(lp)
    linv[...] = jnp.zeros_like(linv)
    ybuf[...] = jnp.zeros_like(ybuf)
    eye = iota((CH, CH), 0) == iota((CH, CH), 1)

    mid = cols // 2

    def diag(i, carry):
        load(i).wait()
        sl = pl.ds(pl.multiple_of(i * lrows, lrows), lrows)
        gacc[:mid, :] += dot(a_v[sl, :mid], a_v[sl, :], 0, 0)
        gacc[mid:, mid:] += dot(a_v[sl, mid:], a_v[sl, mid:], 0, 0)

        def moment(j, c2):
            g = i * (lrows // CH) + j
            brow = jnp.broadcast_to(b_ref[pl.ds(g, 1), :], (CH, CH))
            bcol = jnp.sum(jnp.where(eye, brow, 0.0), axis=1, keepdims=True)
            blk = a_v[pl.ds(pl.multiple_of(g * CH, CH), CH), :]
            hacc[...] += jnp.sum((blk * bcol).reshape(CH // 8, 8, cols), axis=0)
            return c2

        return lax.fori_loop(0, lrows // CH, moment, carry)

    lax.fori_loop(0, nload, diag, 0)
    gacc[mid:, :mid] = gacc[:mid, mid:].T

    pr = cols // GROUPS

    def rows_of(p, n):
        return pl.ds(pl.multiple_of(p * n, n), n)

    def diag_send(off):
        p = peer(off)
        return remote(gacc.at[rows_of(p, pr), :], drecv.at[off - 1], ds_sem.at[off - 1], dr_sem.at[off - 1], t, p)

    def mom_send(off):
        return remote(hacc, hrecv.at[d], hs_sem.at[off - 1], hr_sem.at[off - 1], t, peer(off))

    def mom_arrive(off):
        src = lax.rem(d + GROUPS - off, GROUPS)
        return remote(hacc, hrecv.at[src], hs_sem.at[off - 1], hr_sem.at[off - 1], t, peer(off))

    for off in range(1, GROUPS):
        diag_send(off).start()
        mom_send(off).start()
    hrecv[d] = hacc[...]

    cr = CH // GROUPS

    def cross(k):
        cacc[...] = jnp.zeros_like(cacc)

        def step(s, carry):
            sl = pl.ds(pl.multiple_of(s * srows, srows), srows)
            buf = xr.at[k % SLOTS, sl, :]
            remote(buf, buf, xs_sem.at[k, s], xr_sem.at[k, s], other, d).wait_recv()
            mine = a_v[pl.ds(pl.multiple_of(t * half + s * srows, srows), srows), :]
            cacc[...] += dot(xr[k % SLOTS, sl, :], mine, 0, 0)
            return carry

        lax.fori_loop(0, subs, step, 0)

    def cross_send(k, off):
        p = peer(off)
        return remote(cacc.at[rows_of(p, cr), :], crecv.at[k, off - 1], rs_sem.at[k, off - 1], rr_sem.at[k, off - 1], t, p)

    def spread(ref, n, ssem, rsem, slot, off):
        if slot == 7:
            return remote(ref.at[t, rows_of(d, n), :], ref.at[t, rows_of(d, n), :], ssem.at[7], rsem.at[7], other, d)
        plane = t if slot < 7 else other
        return remote(
            ref.at[plane, rows_of(d, n), :], ref.at[plane, rows_of(d, n), :], ssem.at[slot], rsem.at[slot], t, peer(off)
        )

    def arrive(ref, n, ssem, rsem, slot, off):
        if slot == 7:
            piece = ref.at[other, rows_of(d, n), :]
            return remote(piece, piece, ssem.at[7], rsem.at[7], other, d)
        src = lax.rem(d + GROUPS - off, GROUPS)
        piece = ref.at[t if slot < 7 else other, rows_of(src, n), :]
        return remote(piece, piece, ssem.at[slot], rsem.at[slot], t, peer(off))

    def gather_start(ref, n, ssem, rsem):
        spread(ref, n, ssem, rsem, 7, 0).start()
        for off in range(1, GROUPS):
            spread(ref, n, ssem, rsem, off - 1, off).start()

    def gather_finish(ref, n, ssem, rsem):
        arrive(ref, n, ssem, rsem, 7, 0).wait_recv()
        for off in range(1, GROUPS):
            spread(ref, n, ssem, rsem, 7 + off, off).start()
        for off in range(1, GROUPS):
            arrive(ref, n, ssem, rsem, off - 1, off).wait_recv()
        for off in range(1, GROUPS):
            arrive(ref, n, ssem, rsem, 7 + off, off).wait_recv()
        for slot in range(7):
            spread(ref, n, ssem, rsem, slot, slot + 1).wait_send()
        spread(ref, n, ssem, rsem, 7, 0).wait_send()
        for off in range(1, GROUPS):
            spread(ref, n, ssem, rsem, 7 + off, off).wait_send()

    def cross_reduce(k):
        for off in range(1, GROUPS):
            cross_send(k, off).start()
        acc = cacc[rows_of(d, cr), :]
        for off in range(1, GROUPS):
            cross_send(k, off).wait_recv()
            acc = acc + crecv[k, off - 1]
        cg[k, t, rows_of(d, cr), :] = acc
        for off in range(1, GROUPS):
            cross_send(k, off).wait_send()

    def diag_reduce():
        acc = gacc[rows_of(d, pr), :]
        for off in range(1, GROUPS):
            diag_send(off).wait_recv()
            acc = acc + drecv[off - 1]
        gall[t, rows_of(d, pr), :] = acc
        for off in range(1, GROUPS):
            mom_arrive(off).wait_recv()
        mom = hrecv[0]
        for p in range(1, GROUPS):
            mom = mom + hrecv[p]
        hall[t] = mom
        for off in range(1, GROUPS):
            diag_send(off).wait_send()
            mom_send(off).wait_send()

    def mom_swap(plane):
        piece = hall.at[plane]
        return remote(piece, piece, hs_sem.at[7], hr_sem.at[7], other, d)

    def factor(k):
        wide = 2 * CH
        for tr in range(2):
            for j in range(k + 1):
                for tc in range(2):
                    if tr == tc:
                        blk = gall[tr, k * CH : (k + 1) * CH, j * CH : (j + 1) * CH]
                    else:
                        blk = cg[k, tc, :, j * CH : (j + 1) * CH] + cg[j, tr, :, k * CH : (k + 1) * CH].T
                    pan[tr * CH : (tr + 1) * CH, j * wide + tc * CH : j * wide + (tc + 1) * CH] = blk
        low = k * wide
        for n in range(k):
            seen = (n + 1) * wide
            lp[:, n * wide : seen] = dot(pan[:, :seen], linv[n * wide : seen, :seen], 1, 1)
        ridge = lam_ref[0, 0]
        sch = pan[:, low : low + wide] + jnp.where(iota((wide, wide), 0) == iota((wide, wide), 1), ridge, 0.0)
        if k:
            sch = sch - dot(lp[:, :low], lp[:, :low], 1, 1)
        s0[...] = sch[:CH, :CH]
        s10 = sch[CH:, :CH]
        chol_inverse(s0, w0)
        n00 = w0[...]
        l10 = dot(s10, n00, 1, 1)
        s1[...] = sch[CH:, CH:] - dot(l10, l10, 1, 1)
        chol_inverse(s1, w1)
        n11 = w1[...]
        nbuf[:CH, :CH] = n00
        nbuf[:CH, CH:] = jnp.zeros((CH, CH), F32)
        nbuf[CH:, :CH] = -dot(n11, dot(l10, n00, 1, 0), 1, 0)
        nbuf[CH:, CH:] = n11
        rhs = hpos[:, low : low + wide]
        if k:
            rhs = rhs - dot(ybuf[:, :low], lp[:, :low], 1, 1)
        y = dot(rhs, nbuf[...], 1, 1)
        if k == nch - 1:
            return y
        ybuf[:, low : low + wide] = y
        for n in range(k):
            sl = slice(n * wide, (n + 1) * wide)
            part = dot(lp[:, n * wide : low], linv[n * wide : low, sl], 1, 0)
            linv[low : low + wide, sl] = -dot(nbuf[...], part, 1, 0)
        linv[low : low + wide, low : low + wide] = nbuf[...]
        return y

    y = None
    for k in range(nch):
        cross(k)
        if k == 0:
            diag_reduce()
            gather_start(gall, pr, gs_sem.at[nch], gr_sem.at[nch])
            mom_swap(t).start()
        cross_reduce(k)
        gather_start(cg.at[k], cr, gs_sem.at[k], gr_sem.at[k])
        issue(ahead[k], ahead[k + 1])
        gather_finish(cg.at[k], cr, gs_sem.at[k], gr_sem.at[k])
        if k == 0:
            gather_finish(gall, pr, gs_sem.at[nch], gr_sem.at[nch])
            mom_swap(other).wait_recv()
            mom_swap(t).wait_send()
            for tt in range(2):
                hrow = jnp.broadcast_to(jnp.sum(hall[tt], axis=0, keepdims=True), (8, cols))
                for j in range(nch):
                    p = (2 * j + tt) * CH
                    hpos[:, p : p + CH] = hrow[:, j * CH : (j + 1) * CH]
        y = factor(k)

    last = dot(y, nbuf[...], 1, 0)
    rest = dot(ybuf[...] - dot(last, lp[...], 1, 0), linv[...], 1, 0)
    xpos = jnp.concatenate([rest, last], axis=1)
    sides = [
        jnp.concatenate([xpos[0:1, (2 * j + tt) * CH : (2 * j + tt + 1) * CH] for j in range(nch)], axis=1) for tt in range(2)
    ]
    for tt in range(2):
        for j in range(nch):
            x_ref[tt * nch + j : tt * nch + j + 1, :] = sides[tt][:, j * CH : (j + 1) * CH]
    own = jnp.where(t == 0, sides[0], sides[1])

    def fit(g, carry):
        blk = a_v[pl.ds(pl.multiple_of(g * CH, CH), CH), :] * own
        tot = blk[:, :CH]
        for j in range(1, nch):
            tot = tot + blk[:, j * CH : (j + 1) * CH]
        tot = jnp.sum(tot, axis=1, keepdims=True)
        pbuf[pl.ds(g, 1), :] = jnp.sum(jnp.where(eye, tot, 0.0), axis=0, keepdims=True)
        return carry

    ngroup = rows // CH
    parts = ps_sem.shape[0]
    per = ngroup // parts

    def swap(q):
        sl = pl.ds(q * per, per)
        return remote(pbuf.at[sl, :], prec.at[sl, :], ps_sem.at[q], pr_sem.at[q], other, d)

    for q in range(parts):
        lax.fori_loop(q * per, (q + 1) * per, fit, 0)
        swap(q).start()
    for q in range(parts):
        swap(q).wait_recv()
        sl = pl.ds(q * per, per)
        r_ref[sl, :] = b_ref[sl, :] - (pbuf[sl, :] + prec[sl, :])
    for q in range(parts):
        swap(q).wait_send()
    for q in range(total):
        exchange(q).wait_send()


def solution(mesh):
    def local_fit(design, target, ridge):
        rows, cols = design.shape
        half = rows // 2
        nch = cols // CH
        subs = 8
        nload = 16
        wide = 2 * CH
        prev = (nch - 1) * wide
        ngroup = rows // CH
        vm = pltpu.VMEM
        dma = pltpu.SemaphoreType.DMA
        scratch = [
            vm((rows, cols), F32),
            vm((SLOTS, half, CH), F32),
            vm((cols, cols), F32),
            vm((8, cols), F32),
            vm((GROUPS - 1, cols // GROUPS, cols), F32),
            vm((GROUPS, 8, cols), F32),
            vm((2, cols, cols), F32),
            vm((2, 8, cols), F32),
            vm((CH, cols), F32),
            vm((nch, GROUPS - 1, CH // GROUPS, cols), F32),
            vm((nch, 2, CH, cols), F32),
            vm((wide, nch * wide), F32),
            vm((wide, prev), F32),
            vm((prev, prev), F32),
            vm((CH, CH), F32),
            vm((CH, CH), F32),
            vm((CH, CH), F32),
            vm((CH, CH), F32),
            vm((wide, wide), F32),
            vm((8, nch * wide), F32),
            vm((8, prev), F32),
            vm((ngroup, CH), F32),
            vm((ngroup, CH), F32),
            dma((nload,)),
            dma((nch, subs)),
            dma((nch, subs)),
            dma((7,)),
            dma((7,)),
            dma((8,)),
            dma((8,)),
            dma((nch + 1, 15)),
            dma((nch + 1, 15)),
            dma((nch, 7)),
            dma((nch, 7)),
            dma((4,)),
            dma((4,)),
        ]
        x, r = pl.pallas_call(
            kernel,
            out_shape=(jax.ShapeDtypeStruct((2 * nch, CH), F32), jax.ShapeDtypeStruct((ngroup, CH), F32)),
            in_specs=[
                pl.BlockSpec(memory_space=pltpu.SMEM),
                pl.BlockSpec(memory_space=pltpu.VMEM),
                pl.BlockSpec(memory_space=pl.ANY),
            ],
            out_specs=(pl.BlockSpec(memory_space=pltpu.VMEM), pl.BlockSpec(memory_space=pltpu.VMEM)),
            scratch_shapes=scratch,
            compiler_params=pltpu.CompilerParams(collective_id=0, has_side_effects=True, vmem_limit_bytes=67043328),
        )(ridge.reshape(1, 1), target.reshape(ngroup, CH), design)
        return x.reshape(-1), r.reshape(-1)

    return jax.shard_map(
        local_fit, mesh=mesh, in_specs=(P("dp", "tp"), P("dp"), P()), out_specs=(P(), P("dp")), check_vma=False
    )
```

```python
import functools

import jax
import jax.numpy as jnp
from jax import lax
from jax.experimental import pallas as pl
from jax.experimental.pallas import tpu as pltpu
from jax.sharding import PartitionSpec as P

MESH = pl.DeviceIdType.MESH
HIGHEST = lax.Precision.HIGHEST
F32 = jnp.float32
CH = 128
GROUPS = 8
STEP = 8
LAST_STEP = 32
SLOTS = 3


def dot(a, b, ca, cb):
    return lax.dot_general(a, b, (((ca,), (cb,)), ((), ())), precision=HIGHEST, preferred_element_type=F32)


def iota(shape, dim):
    return lax.broadcasted_iota(jnp.int32, shape, dim)


def chol_inverse(s_ref, w_ref, step):
    w_ref[...] = jnp.where(iota((CH, CH), 0) == iota((CH, CH), 1), 1.0, 0.0).astype(F32)
    lane, sub = iota((8, CH), 1), iota((8, CH), 0)
    tiles = step // 8

    def spread(row):
        return jnp.broadcast_to(row, (8, CH))

    def group(g, carry):
        r0 = pl.multiple_of(g * step, step)
        rows = [s_ref[pl.ds(r0 + 8 * a, 8), :] for a in range(tiles)]
        inv = [w_ref[pl.ds(r0 + 8 * a, 8), :] for a in range(tiles)]
        cols = [
            [
                spread(jnp.sum(jnp.where(lane == r0 + i, rows[a], 0.0), axis=1, keepdims=True)) if a >= i // 8 else None
                for a in range(tiles)
            ]
            for i in range(step)
        ]
        for i in range(step):
            a0, r = divmod(i, 8)
            piv = spread(cols[i][a0][r : r + 1, :])
            scale = lax.rsqrt(piv)
            scale = scale * (1.5 - 0.5 * piv * scale * scale)
            u = spread(rows[a0][r : r + 1, :]) * scale
            v = spread(inv[a0][r : r + 1, :]) * scale
            coef = [None] * tiles
            for a in range(a0, tiles):
                c = cols[i][a] * scale
                coef[a] = jnp.where(sub > r, c, 0.0) if a == a0 else c
                down, side = rows[a] - coef[a] * u, inv[a] - coef[a] * v
                rows[a] = jnp.where(sub == r, u, down) if a == a0 else down
                inv[a] = jnp.where(sub == r, v, side) if a == a0 else side
            for j in range(i + 1, step):
                b0, q = divmod(j, 8)
                lead = spread(coef[b0][q : q + 1, :])
                for a in range(b0, tiles):
                    cols[j][a] = cols[j][a] - coef[a] * lead
        for a in range(tiles):
            w_ref[pl.ds(r0 + 8 * a, 8), :] = inv[a]
        panel = jnp.concatenate(rows, axis=0)
        both = jnp.concatenate([panel, jnp.concatenate(inv, axis=0)], axis=1)

        @pl.when(g < CH // step - 1)
        def _():
            below = jnp.where(iota((step, CH), 1) >= r0 + step, panel, 0.0)
            upd = dot(below, both, 0, 0)
            s_ref[...] -= upd[:, :CH]
            w_ref[...] -= upd[:, CH:]

        return carry

    lax.fori_loop(0, CH // step, group, 0)


def kernel(
    lam_ref, b_hbm, a_hbm, x_hbm, r_hbm,
    b_ref, x_ref, r_ref,
    a_v, xr, gacc, hacc, drecv, hrecv, gall, hall, cacc, crecv, cg, pan, lp, linv, s0, s1, w0, nbuf, hpos, ybuf, pbuf, prec,
    small_sem, load_sem, xs_sem, xr_sem, ds_sem, dr_sem, hs_sem, hr_sem, gs_sem, gr_sem, rs_sem, rr_sem, ps_sem, pr_sem, out_sem,
):
    rows, cols = a_v.shape
    half = rows // 2
    nch = cols // CH
    subs = xr_sem.shape[1]
    srows = half // subs
    nload = load_sem.shape[0]
    lrows = rows // nload
    t = lax.axis_index("tp")
    d = lax.axis_index("dp")
    other = 1 - t

    def peer(off):
        return lax.rem(d + off, GROUPS)

    def remote(src, dst, ssem, rsem, tp, dp):
        return pltpu.make_async_remote_copy(
            src_ref=src, dst_ref=dst, send_sem=ssem, recv_sem=rsem, device_id={"tp": tp, "dp": dp}, device_id_type=MESH
        )

    def load(i):
        sl = pl.ds(pl.multiple_of(i * lrows, lrows), lrows)
        return pltpu.make_async_copy(a_hbm.at[sl, :], a_v.at[sl, :], load_sem.at[i])

    barrier = pltpu.get_barrier_semaphore()
    pl.semaphore_signal(barrier, inc=1, device_id={"tp": other, "dp": d}, device_id_type=MESH)
    for off in range(1, GROUPS):
        pl.semaphore_signal(barrier, inc=1, device_id={"tp": t, "dp": peer(off)}, device_id_type=MESH)
    for i in range(nload):
        load(i).start()
    pl.semaphore_wait(barrier, GROUPS)

    def exchange(q):
        c, s = q // subs, q % subs
        src = a_hbm.at[pl.ds(pl.multiple_of(other * half + s * srows, srows), srows), pl.ds(c * CH, CH)]
        return remote(src, xr.at[c % SLOTS, pl.ds(s * srows, srows), :], xs_sem.at[c, s], xr_sem.at[c, s], other, d)

    def issue(lo, hi):
        for q in range(lo, hi):
            exchange(q).start()

    total = nch * subs
    ahead = [subs + 3] + [min((k + 2) * subs + 2, total) for k in range(nch)]
    issue(0, ahead[0])
    b_in = pltpu.make_async_copy(b_hbm, b_ref, small_sem.at[0])
    b_in.start()

    gacc[...] = jnp.zeros_like(gacc)
    hacc[...] = jnp.zeros_like(hacc)
    pan[...] = jnp.zeros_like(pan)
    lp[...] = jnp.zeros_like(lp)
    linv[...] = jnp.zeros_like(linv)
    ybuf[...] = jnp.zeros_like(ybuf)
    eye = iota((CH, CH), 0) == iota((CH, CH), 1)

    b_in.wait()

    mid = cols // 2

    def diag(i, carry):
        load(i).wait()
        sl = pl.ds(pl.multiple_of(i * lrows, lrows), lrows)
        gacc[:mid, :] += dot(a_v[sl, :mid], a_v[sl, :], 0, 0)
        gacc[mid:, mid:] += dot(a_v[sl, mid:], a_v[sl, mid:], 0, 0)

        def moment(j, c2):
            g = i * (lrows // CH) + j
            brow = jnp.broadcast_to(b_ref[pl.ds(g, 1), :], (CH, CH))
            bcol = jnp.sum(jnp.where(eye, brow, 0.0), axis=1, keepdims=True)
            blk = a_v[pl.ds(pl.multiple_of(g * CH, CH), CH), :]
            hacc[...] += jnp.sum((blk * bcol).reshape(CH // 8, 8, cols), axis=0)
            return c2

        return lax.fori_loop(0, lrows // CH, moment, carry)

    lax.fori_loop(0, nload, diag, 0)
    gacc[mid:, :mid] = gacc[:mid, mid:].T

    pr = cols // GROUPS

    def rows_of(p, n):
        return pl.ds(pl.multiple_of(p * n, n), n)

    def diag_send(off):
        p = peer(off)
        return remote(gacc.at[rows_of(p, pr), :], drecv.at[off - 1], ds_sem.at[off - 1], dr_sem.at[off - 1], t, p)

    def mom_send(off):
        return remote(hacc, hrecv.at[d], hs_sem.at[off - 1], hr_sem.at[off - 1], t, peer(off))

    def mom_arrive(off):
        src = lax.rem(d + GROUPS - off, GROUPS)
        return remote(hacc, hrecv.at[src], hs_sem.at[off - 1], hr_sem.at[off - 1], t, peer(off))

    for off in range(1, GROUPS):
        diag_send(off).start()
        mom_send(off).start()
    hrecv[d] = hacc[...]

    cr = CH // GROUPS

    def cross(k):
        cacc[...] = jnp.zeros_like(cacc)

        def step(s, carry):
            sl = pl.ds(pl.multiple_of(s * srows, srows), srows)
            buf = xr.at[k % SLOTS, sl, :]
            remote(buf, buf, xs_sem.at[k, s], xr_sem.at[k, s], other, d).wait_recv()
            mine = a_v[pl.ds(pl.multiple_of(t * half + s * srows, srows), srows), :]
            cacc[...] += dot(xr[k % SLOTS, sl, :], mine, 0, 0)
            return carry

        lax.fori_loop(0, subs, step, 0)

    def cross_send(k, off):
        p = peer(off)
        return remote(cacc.at[rows_of(p, cr), :], crecv.at[k, off - 1], rs_sem.at[k, off - 1], rr_sem.at[k, off - 1], t, p)

    def spread(ref, n, ssem, rsem, slot, off):
        if slot == 7:
            return remote(ref.at[t, rows_of(d, n), :], ref.at[t, rows_of(d, n), :], ssem.at[7], rsem.at[7], other, d)
        plane = t if slot < 7 else other
        return remote(
            ref.at[plane, rows_of(d, n), :], ref.at[plane, rows_of(d, n), :], ssem.at[slot], rsem.at[slot], t, peer(off)
        )

    def arrive(ref, n, ssem, rsem, slot, off):
        if slot == 7:
            piece = ref.at[other, rows_of(d, n), :]
            return remote(piece, piece, ssem.at[7], rsem.at[7], other, d)
        src = lax.rem(d + GROUPS - off, GROUPS)
        piece = ref.at[t if slot < 7 else other, rows_of(src, n), :]
        return remote(piece, piece, ssem.at[slot], rsem.at[slot], t, peer(off))

    def gather_start(ref, n, ssem, rsem):
        spread(ref, n, ssem, rsem, 7, 0).start()
        for off in range(1, GROUPS):
            spread(ref, n, ssem, rsem, off - 1, off).start()

    def gather_finish(ref, n, ssem, rsem):
        arrive(ref, n, ssem, rsem, 7, 0).wait_recv()
        for off in range(1, GROUPS):
            spread(ref, n, ssem, rsem, 7 + off, off).start()
        for off in range(1, GROUPS):
            arrive(ref, n, ssem, rsem, off - 1, off).wait_recv()
        for off in range(1, GROUPS):
            arrive(ref, n, ssem, rsem, 7 + off, off).wait_recv()
        for slot in range(7):
            spread(ref, n, ssem, rsem, slot, slot + 1).wait_send()
        spread(ref, n, ssem, rsem, 7, 0).wait_send()
        for off in range(1, GROUPS):
            spread(ref, n, ssem, rsem, 7 + off, off).wait_send()

    def cross_reduce(k):
        for off in range(1, GROUPS):
            cross_send(k, off).start()
        acc = cacc[rows_of(d, cr), :]
        for off in range(1, GROUPS):
            cross_send(k, off).wait_recv()
            acc = acc + crecv[k, off - 1]
        cg[k, t, rows_of(d, cr), :] = acc
        for off in range(1, GROUPS):
            cross_send(k, off).wait_send()

    def diag_reduce():
        acc = gacc[rows_of(d, pr), :]
        for off in range(1, GROUPS):
            diag_send(off).wait_recv()
            acc = acc + drecv[off - 1]
        gall[t, rows_of(d, pr), :] = acc
        for off in range(1, GROUPS):
            mom_arrive(off).wait_recv()
        mom = hrecv[0]
        for p in range(1, GROUPS):
            mom = mom + hrecv[p]
        hall[t] = mom
        for off in range(1, GROUPS):
            diag_send(off).wait_send()
            mom_send(off).wait_send()

    def mom_swap(plane):
        piece = hall.at[plane]
        return remote(piece, piece, hs_sem.at[7], hr_sem.at[7], other, d)

    wide = 2 * CH

    def pan_at(tr, tc, j):
        return slice(tr * CH, (tr + 1) * CH), slice(j * wide + tc * CH, j * wide + (tc + 1) * CH)

    def prepare(k):
        for tr in range(2):
            for j in range(k + 1):
                pan[pan_at(tr, tr, j)] = gall[tr, k * CH : (k + 1) * CH, j * CH : (j + 1) * CH]
                if j < k:
                    pan[pan_at(tr, 1 - tr, j)] = cg[j, tr, :, k * CH : (k + 1) * CH].T

    def factor(k):
        for tr in range(2):
            for j in range(k):
                pan[pan_at(tr, 1 - tr, j)] += cg[k, 1 - tr, :, j * CH : (j + 1) * CH]
        here = slice(k * CH, (k + 1) * CH)
        pan[pan_at(1, 0, k)] = cg[k, 0, :, here] + cg[k, 1, :, here].T
        low = k * wide
        for n in range(k):
            seen = (n + 1) * wide
            lp[:, n * wide : seen] = dot(pan[:, :seen], linv[n * wide : seen, :seen], 1, 1)
        ridge = lam_ref[0, 0]
        sch = pan[:, low : low + wide] + jnp.where(iota((wide, wide), 0) == iota((wide, wide), 1), ridge, 0.0)
        if k:
            sch = sch - dot(lp[:, :low], lp[:, :low], 1, 1)
        s0[0] = sch[:CH, :CH]
        s1[...] = sch[CH:, :]

        def block(h, carry):
            @pl.when(h == 1)
            def _():
                l10 = dot(s1[:, :CH], w0[0], 1, 1)
                s0[1] = s1[:, CH:] - dot(l10, l10, 1, 1)
                s1[:, :CH] = l10

            chol_inverse(s0.at[h], w0.at[h], STEP if k < nch - 1 else LAST_STEP)
            return carry

        lax.fori_loop(0, 2, block, 0)
        n00, n11 = w0[0], w0[1]
        nbuf[:CH, :CH] = n00
        nbuf[:CH, CH:] = jnp.zeros((CH, CH), F32)
        nbuf[CH:, :CH] = -dot(n11, dot(s1[:, :CH], n00, 1, 0), 1, 0)
        nbuf[CH:, CH:] = n11
        if k == nch - 1:
            return
        rhs = hpos[:, low : low + wide]
        if k:
            rhs = rhs - dot(ybuf[:, :low], lp[:, :low], 1, 1)
        y = dot(rhs, nbuf[...], 1, 1)
        ybuf[:, low : low + wide] = y
        for n in range(k):
            sl = slice(n * wide, (n + 1) * wide)
            part = dot(lp[:, n * wide : low], linv[n * wide : low, sl], 1, 0)
            linv[low : low + wide, sl] = -dot(nbuf[...], part, 1, 0)
        linv[low : low + wide, low : low + wide] = nbuf[...]

    for k in range(nch):
        if k:
            prepare(k)
        cross(k)
        if k == 0:
            diag_reduce()
            gather_start(gall, pr, gs_sem.at[nch], gr_sem.at[nch])
            mom_swap(t).start()
        cross_reduce(k)
        gather_start(cg.at[k], cr, gs_sem.at[k], gr_sem.at[k])
        issue(ahead[k], ahead[k + 1])
        gather_finish(cg.at[k], cr, gs_sem.at[k], gr_sem.at[k])
        if k == 0:
            gather_finish(gall, pr, gs_sem.at[nch], gr_sem.at[nch])
            mom_swap(other).wait_recv()
            mom_swap(t).wait_send()
            for tt in range(2):
                hrow = jnp.broadcast_to(jnp.sum(hall[tt], axis=0, keepdims=True), (8, cols))
                for j in range(nch):
                    p = (2 * j + tt) * CH
                    hpos[:, p : p + CH] = hrow[:, j * CH : (j + 1) * CH]
            prepare(0)
        factor(k)

    def to_row(col):
        n = col.shape[0] // CH
        return jnp.concatenate(
            [jnp.sum(jnp.where(eye, col[i * CH : (i + 1) * CH], 0.0), axis=0, keepdims=True) for i in range(n)], axis=1
        )

    def to_col(row):
        n = row.shape[1] // CH
        return jnp.concatenate(
            [jnp.sum(jnp.where(eye, row[:, i * CH : (i + 1) * CH], 0.0), axis=1, keepdims=True) for i in range(n)], axis=0
        )

    def down(mat, col):
        return jnp.sum(mat * col, axis=0, keepdims=True)

    prev = (nch - 1) * wide
    seen = jnp.sum(lp[...] * ybuf[0:1, :], axis=1, keepdims=True)
    rhs = hpos[0:1, prev:] - to_row(seen)
    ycol = jnp.sum(nbuf[...] * rhs, axis=1, keepdims=True)
    last = down(nbuf[...], ycol)
    ucol = to_col(ybuf[0:1, :] - down(lp[...], to_col(last)))
    rest = [down(linv[n * wide :, n * wide : (n + 1) * wide], ucol[n * wide :]) for n in range(nch - 1)]
    xpos = jnp.concatenate(rest + [last], axis=1)
    sides = [
        jnp.concatenate([xpos[0:1, (2 * j + tt) * CH : (2 * j + tt + 1) * CH] for j in range(nch)], axis=1) for tt in range(2)
    ]
    for tt in range(2):
        for j in range(nch):
            x_ref[tt * nch + j : tt * nch + j + 1, :] = sides[tt][:, j * CH : (j + 1) * CH]
    own = jnp.where(t == 0, sides[0], sides[1])
    x_out = pltpu.make_async_copy(x_ref, x_hbm, small_sem.at[1])
    x_out.start()

    def fit(m, carry):
        for g in range(8):
            blk = a_v[pl.ds(pl.multiple_of((m * 8 + g) * CH, CH), CH), :] * own
            tot = blk[:, :CH]
            for j in range(1, nch):
                tot = tot + blk[:, j * CH : (j + 1) * CH]
            tot = jnp.sum(tot, axis=1, keepdims=True)
            pbuf[pl.ds(m * 8 + g, 1), :] = jnp.sum(jnp.where(eye, tot, 0.0), axis=0, keepdims=True)
        return carry

    ngroup = rows // CH
    parts = ps_sem.shape[0]
    per = ngroup // parts

    def swap(q):
        sl = pl.ds(q * per, per)
        return remote(pbuf.at[sl, :], prec.at[sl, :], ps_sem.at[q], pr_sem.at[q], other, d)

    def r_out(q):
        sl = pl.ds(q * per, per)
        return pltpu.make_async_copy(r_ref.at[sl, :], r_hbm.at[sl, :], out_sem.at[q])

    for q in range(parts):
        lax.fori_loop(q * per // 8, (q + 1) * per // 8, fit, 0)
        swap(q).start()
    for q in range(parts):
        swap(q).wait_recv()
        sl = pl.ds(q * per, per)
        r_ref[sl, :] = b_ref[sl, :] - (pbuf[sl, :] + prec[sl, :])
        r_out(q).start()
    for q in range(parts):
        swap(q).wait_send()
    for q in range(total):
        exchange(q).wait_send()
    x_out.wait()
    for q in range(parts):
        r_out(q).wait()


def solution(mesh):
    def local_fit(design, target, ridge):
        rows, cols = design.shape
        half = rows // 2
        nch = cols // CH
        subs = 8
        nload = 16
        wide = 2 * CH
        prev = (nch - 1) * wide
        ngroup = rows // CH
        vm = pltpu.VMEM
        dma = pltpu.SemaphoreType.DMA
        scratch = [
            vm((ngroup, CH), F32),
            vm((2 * nch, CH), F32),
            vm((ngroup, CH), F32),
            vm((rows, cols), F32),
            vm((SLOTS, half, CH), F32),
            vm((cols, cols), F32),
            vm((8, cols), F32),
            vm((GROUPS - 1, cols // GROUPS, cols), F32),
            vm((GROUPS, 8, cols), F32),
            vm((2, cols, cols), F32),
            vm((2, 8, cols), F32),
            vm((CH, cols), F32),
            vm((nch, GROUPS - 1, CH // GROUPS, cols), F32),
            vm((nch, 2, CH, cols), F32),
            vm((wide, nch * wide), F32),
            vm((wide, prev), F32),
            vm((prev, prev), F32),
            vm((2, CH, CH), F32),
            vm((CH, wide), F32),
            vm((2, CH, CH), F32),
            vm((wide, wide), F32),
            vm((8, nch * wide), F32),
            vm((8, prev), F32),
            vm((ngroup, CH), F32),
            vm((ngroup, CH), F32),
            dma((2,)),
            dma((nload,)),
            dma((nch, subs)),
            dma((nch, subs)),
            dma((7,)),
            dma((7,)),
            dma((8,)),
            dma((8,)),
            dma((nch + 1, 15)),
            dma((nch + 1, 15)),
            dma((nch, 7)),
            dma((nch, 7)),
            dma((4,)),
            dma((4,)),
            dma((4,)),
        ]
        x, r = pl.pallas_call(
            kernel,
            out_shape=(jax.ShapeDtypeStruct((2 * nch, CH), F32), jax.ShapeDtypeStruct((ngroup, CH), F32)),
            in_specs=[pl.BlockSpec(memory_space=pltpu.SMEM)] + [pl.BlockSpec(memory_space=pl.ANY)] * 2,
            out_specs=(pl.BlockSpec(memory_space=pl.ANY), pl.BlockSpec(memory_space=pl.ANY)),
            scratch_shapes=scratch,
            compiler_params=pltpu.CompilerParams(collective_id=0, has_side_effects=True, vmem_limit_bytes=67043328),
        )(ridge.reshape(1, 1), target.reshape(ngroup, CH), design)
        def emit(xi, ri, xo, ro):
            xo[...] = xi[...]
            ro[...] = ri[...]

        x, r = pl.pallas_call(
            emit,
            out_shape=(jax.ShapeDtypeStruct((2 * nch, CH), F32), jax.ShapeDtypeStruct((ngroup, CH), F32)),
        )(x, r)
        return x.reshape(-1), r.reshape(-1)

    return jax.shard_map(
        local_fit, mesh=mesh, in_specs=(P("dp", "tp"), P("dp"), P()), out_specs=(P(), P("dp")), check_vma=False
    )
```

```python
import functools

import jax
import jax.numpy as jnp
from jax import lax
from jax.experimental import pallas as pl
from jax.experimental.pallas import tpu as pltpu
from jax.sharding import PartitionSpec as P

MESH = pl.DeviceIdType.MESH
HIGHEST = lax.Precision.HIGHEST
F32 = jnp.float32
CH = 128
GROUPS = 8
STEP = 8
LAST_STEP = 32
SLOTS = 3


def dot(a, b, ca, cb):
    return lax.dot_general(a, b, (((ca,), (cb,)), ((), ())), precision=HIGHEST, preferred_element_type=F32)


def iota(shape, dim):
    return lax.broadcasted_iota(jnp.int32, shape, dim)


def chol_inverse(s_ref, w_ref, step):
    w_ref[...] = jnp.where(iota((CH, CH), 0) == iota((CH, CH), 1), 1.0, 0.0).astype(F32)
    lane, sub = iota((8, CH), 1), iota((8, CH), 0)
    tiles = step // 8

    def spread(row):
        return jnp.broadcast_to(row, (8, CH))

    def group(g, carry):
        r0 = pl.multiple_of(g * step, step)
        rows = [s_ref[pl.ds(r0 + 8 * a, 8), :] for a in range(tiles)]
        inv = [w_ref[pl.ds(r0 + 8 * a, 8), :] for a in range(tiles)]
        cols = [
            [
                spread(jnp.sum(jnp.where(lane == r0 + i, rows[a], 0.0), axis=1, keepdims=True)) if a >= i // 8 else None
                for a in range(tiles)
            ]
            for i in range(step)
        ]
        for i in range(step):
            a0, r = divmod(i, 8)
            piv = spread(cols[i][a0][r : r + 1, :])
            scale = lax.rsqrt(piv)
            scale = scale * (1.5 - 0.5 * piv * scale * scale)
            u = spread(rows[a0][r : r + 1, :]) * scale
            v = spread(inv[a0][r : r + 1, :]) * scale
            coef = [None] * tiles
            for a in range(a0, tiles):
                c = cols[i][a] * scale
                coef[a] = jnp.where(sub > r, c, 0.0) if a == a0 else c
                down, side = rows[a] - coef[a] * u, inv[a] - coef[a] * v
                rows[a] = jnp.where(sub == r, u, down) if a == a0 else down
                inv[a] = jnp.where(sub == r, v, side) if a == a0 else side
            for j in range(i + 1, step):
                b0, q = divmod(j, 8)
                lead = spread(coef[b0][q : q + 1, :])
                for a in range(b0, tiles):
                    cols[j][a] = cols[j][a] - coef[a] * lead
        for a in range(tiles):
            w_ref[pl.ds(r0 + 8 * a, 8), :] = inv[a]
        panel = jnp.concatenate(rows, axis=0)
        both = jnp.concatenate([panel, jnp.concatenate(inv, axis=0)], axis=1)

        @pl.when(g < CH // step - 1)
        def _():
            below = jnp.where(iota((step, CH), 1) >= r0 + step, panel, 0.0)
            upd = dot(below, both, 0, 0)
            s_ref[...] -= upd[:, :CH]
            w_ref[...] -= upd[:, CH:]

        return carry

    lax.fori_loop(0, CH // step, group, 0)


def kernel(
    lam_hbm, b_hbm, a_hbm, x_hbm, r_hbm,
    lam_ref, b_ref, x_ref, x_two, r_ref,
    a_v, xr, gacc, hacc, drecv, hrecv, gall, hall, cacc, crecv, cg, pan, lp, linv, s0, s1, w0, nbuf, hpos, ybuf, pbuf, prec,
    small_sem, load_sem, xs_sem, xr_sem, ds_sem, dr_sem, hs_sem, hr_sem, gs_sem, gr_sem, rs_sem, rr_sem, ps_sem, pr_sem, out_sem, xx_sem,
):
    rows, cols = a_v.shape
    half = rows // 2
    nch = cols // CH
    subs = xr_sem.shape[1]
    srows = half // subs
    nload = load_sem.shape[0]
    lrows = rows // nload
    t = lax.axis_index("tp")
    d = lax.axis_index("dp")
    other = 1 - t

    def peer(off):
        return lax.rem(d + off, GROUPS)

    def remote(src, dst, ssem, rsem, tp, dp):
        return pltpu.make_async_remote_copy(
            src_ref=src, dst_ref=dst, send_sem=ssem, recv_sem=rsem, device_id={"tp": tp, "dp": dp}, device_id_type=MESH
        )

    def load(i):
        sl = pl.ds(pl.multiple_of(i * lrows, lrows), lrows)
        return pltpu.make_async_copy(a_hbm.at[sl, :], a_v.at[sl, :], load_sem.at[i])

    barrier = pltpu.get_barrier_semaphore()
    pl.semaphore_signal(barrier, inc=1, device_id={"tp": other, "dp": d}, device_id_type=MESH)
    for off in range(1, GROUPS):
        pl.semaphore_signal(barrier, inc=1, device_id={"tp": t, "dp": peer(off)}, device_id_type=MESH)
    for i in range(nload):
        load(i).start()
    pl.semaphore_wait(barrier, GROUPS)

    def exchange(q):
        c, s = q // subs, q % subs
        src = a_hbm.at[pl.ds(pl.multiple_of(other * half + s * srows, srows), srows), pl.ds(c * CH, CH)]
        return remote(src, xr.at[c % SLOTS, pl.ds(s * srows, srows), :], xs_sem.at[c, s], xr_sem.at[c, s], other, d)

    def issue(lo, hi):
        for q in range(lo, hi):
            exchange(q).start()

    total = nch * subs
    ahead = [subs + 3] + [min((k + 2) * subs + 2, total) for k in range(nch)]
    issue(0, ahead[0])
    b_in = pltpu.make_async_copy(b_hbm, b_ref, small_sem.at[0])
    b_in.start()
    lam_in = pltpu.make_async_copy(lam_hbm, lam_ref, small_sem.at[2])
    lam_in.start()

    gacc[...] = jnp.zeros_like(gacc)
    hacc[...] = jnp.zeros_like(hacc)
    pan[...] = jnp.zeros_like(pan)
    lp[...] = jnp.zeros_like(lp)
    linv[...] = jnp.zeros_like(linv)
    ybuf[...] = jnp.zeros_like(ybuf)
    eye = iota((CH, CH), 0) == iota((CH, CH), 1)

    b_in.wait()
    lam_in.wait()

    mid = cols // 2

    def diag(i, carry):
        load(i).wait()
        sl = pl.ds(pl.multiple_of(i * lrows, lrows), lrows)
        gacc[:mid, :] += dot(a_v[sl, :mid], a_v[sl, :], 0, 0)
        gacc[mid:, mid:] += dot(a_v[sl, mid:], a_v[sl, mid:], 0, 0)

        def moment(j, c2):
            g = i * (lrows // CH) + j
            brow = jnp.broadcast_to(b_ref[pl.ds(g, 1), :], (CH, CH))
            bcol = jnp.sum(jnp.where(eye, brow, 0.0), axis=1, keepdims=True)
            blk = a_v[pl.ds(pl.multiple_of(g * CH, CH), CH), :]
            hacc[...] += jnp.sum((blk * bcol).reshape(CH // 8, 8, cols), axis=0)
            return c2

        return lax.fori_loop(0, lrows // CH, moment, carry)

    lax.fori_loop(0, nload, diag, 0)
    gacc[mid:, :mid] = gacc[:mid, mid:].T

    pr = cols // GROUPS

    def rows_of(p, n):
        return pl.ds(pl.multiple_of(p * n, n), n)

    def part(p):
        core = lax.rem(p, 2)
        return core * (GROUPS - 1 - p // 2) + (1 - core) * (p // 2)

    def diag_send(off):
        p = peer(off)
        return remote(gacc.at[rows_of(part(p), pr), :], drecv.at[off - 1], ds_sem.at[off - 1], dr_sem.at[off - 1], t, p)

    def mom_send(off):
        return remote(hacc, hrecv.at[d], hs_sem.at[off - 1], hr_sem.at[off - 1], t, peer(off))

    def mom_arrive(off):
        src = lax.rem(d + GROUPS - off, GROUPS)
        return remote(hacc, hrecv.at[src], hs_sem.at[off - 1], hr_sem.at[off - 1], t, peer(off))

    for off in range(1, GROUPS):
        diag_send(off).start()
        mom_send(off).start()
    hrecv[d] = hacc[...]

    cr = CH // GROUPS

    def cross(k):
        cacc[...] = jnp.zeros_like(cacc)

        def step(s, carry):
            sl = pl.ds(pl.multiple_of(s * srows, srows), srows)
            buf = xr.at[k % SLOTS, sl, :]
            remote(buf, buf, xs_sem.at[k, s], xr_sem.at[k, s], other, d).wait_recv()
            mine = a_v[pl.ds(pl.multiple_of(t * half + s * srows, srows), srows), :]
            cacc[...] += dot(xr[k % SLOTS, sl, :], mine, 0, 0)
            return carry

        lax.fori_loop(0, subs, step, 0)

    def cross_send(k, off):
        p = peer(off)
        return remote(cacc.at[rows_of(p, cr), :], crecv.at[k, off - 1], rs_sem.at[k, off - 1], rr_sem.at[k, off - 1], t, p)

    def piece(ref, plane, p):
        n = pr if ref is gall else cr
        return ref.at[plane, rows_of(part(p) if ref is gall else p, n), :]

    def spread(ref, ssem, rsem, slot, off):
        mine = piece(ref, t if slot < 7 else other, d)
        return remote(mine, mine, ssem.at[slot], rsem.at[slot], t, peer(off))

    def arrive(ref, ssem, rsem, slot, off):
        theirs = piece(ref, t if slot < 7 else other, lax.rem(d + GROUPS - off, GROUPS))
        return remote(theirs, theirs, ssem.at[slot], rsem.at[slot], t, peer(off))

    def across(ref, ssem, rsem, plane, act):
        mine = piece(ref, plane, d)
        if ref is not gall:
            act(remote(mine, mine, ssem.at[7], rsem.at[7], other, d))
            return
        for j in range(nch):

            @pl.when(part(d) // 2 == j)
            def _():
                low = gall.at[plane, rows_of(part(d), pr), : (j + 1) * CH]
                act(remote(low, low, ssem.at[7], rsem.at[7], other, d))

    def gather_start(ref, ssem, rsem):
        across(ref, ssem, rsem, t, lambda c: c.start())
        for off in range(1, GROUPS):
            spread(ref, ssem, rsem, off - 1, off).start()

    def gather_plane(ref, ssem, rsem):
        across(ref, ssem, rsem, other, lambda c: c.wait_recv())
        for off in range(1, GROUPS):
            spread(ref, ssem, rsem, 7 + off, off).start()
        for off in range(1, GROUPS):
            arrive(ref, ssem, rsem, off - 1, off).wait_recv()

    def gather_rest(ref, ssem, rsem):
        for off in range(1, GROUPS):
            arrive(ref, ssem, rsem, 7 + off, off).wait_recv()
        for off in range(1, GROUPS):
            spread(ref, ssem, rsem, off - 1, off).wait_send()
        across(ref, ssem, rsem, t, lambda c: c.wait_send())
        for off in range(1, GROUPS):
            spread(ref, ssem, rsem, 7 + off, off).wait_send()

    def gather_finish(ref, ssem, rsem):
        gather_plane(ref, ssem, rsem)
        gather_rest(ref, ssem, rsem)

    def cross_reduce(k):
        for off in range(1, GROUPS):
            cross_send(k, off).start()
        acc = cacc[rows_of(d, cr), :]
        for off in range(1, GROUPS):
            cross_send(k, off).wait_recv()
            acc = acc + crecv[k, off - 1]
        cg[k, t, rows_of(d, cr), :] = acc
        for off in range(1, GROUPS):
            cross_send(k, off).wait_send()

    def diag_reduce():
        acc = gacc[rows_of(part(d), pr), :]
        for off in range(1, GROUPS):
            diag_send(off).wait_recv()
            acc = acc + drecv[off - 1]
        gall[t, rows_of(part(d), pr), :] = acc
        for off in range(1, GROUPS):
            mom_arrive(off).wait_recv()
        mom = hrecv[0]
        for p in range(1, GROUPS):
            mom = mom + hrecv[p]
        hall[t] = mom
        for off in range(1, GROUPS):
            diag_send(off).wait_send()
            mom_send(off).wait_send()

    def mom_swap(plane):
        piece = hall.at[plane]
        return remote(piece, piece, hs_sem.at[7], hr_sem.at[7], other, d)

    wide = 2 * CH

    def pan_at(tr, tc, j):
        return slice(tr * CH, (tr + 1) * CH), slice(j * wide + tc * CH, j * wide + (tc + 1) * CH)

    def prepare(k):
        for tr in range(2):
            for j in range(k + 1):
                pan[pan_at(tr, tr, j)] = gall[tr, k * CH : (k + 1) * CH, j * CH : (j + 1) * CH]
                if j < k:
                    pan[pan_at(tr, 1 - tr, j)] = cg[j, tr, :, k * CH : (k + 1) * CH].T

    def factor(k):
        for tr in range(2):
            for j in range(k):
                pan[pan_at(tr, 1 - tr, j)] += cg[k, 1 - tr, :, j * CH : (j + 1) * CH]
        here = slice(k * CH, (k + 1) * CH)
        pan[pan_at(1, 0, k)] = cg[k, 0, :, here] + cg[k, 1, :, here].T
        low = k * wide
        for n in range(k):
            seen = (n + 1) * wide
            lp[:, n * wide : seen] = dot(pan[:, :seen], linv[n * wide : seen, :seen], 1, 1)
        ridge = lam_ref[0]
        sch = pan[:, low : low + wide] + jnp.where(iota((wide, wide), 0) == iota((wide, wide), 1), ridge, 0.0)
        if k:
            sch = sch - dot(lp[:, :low], lp[:, :low], 1, 1)
        s0[0] = sch[:CH, :CH]
        s1[...] = sch[CH:, :]

        def block(h, carry):
            @pl.when(h == 1)
            def _():
                l10 = dot(s1[:, :CH], w0[0], 1, 1)
                s0[1] = s1[:, CH:] - dot(l10, l10, 1, 1)
                s1[:, :CH] = l10

            chol_inverse(s0.at[h], w0.at[h], STEP)
            return carry

        lax.fori_loop(0, 2, block, 0)
        n00, n11 = w0[0], w0[1]
        nbuf[:CH, :CH] = n00
        nbuf[:CH, CH:] = jnp.zeros((CH, CH), F32)
        nbuf[CH:, :CH] = -dot(n11, dot(s1[:, :CH], n00, 1, 0), 1, 0)
        nbuf[CH:, CH:] = n11
        rhs = hpos[:, low : low + wide]
        if k:
            rhs = rhs - dot(ybuf[:, :low], lp[:, :low], 1, 1)
        y = dot(rhs, nbuf[...], 1, 1)
        ybuf[:, low : low + wide] = y
        for n in range(k):
            sl = slice(n * wide, (n + 1) * wide)
            part = dot(lp[:, n * wide : low], linv[n * wide : low, sl], 1, 0)
            linv[low : low + wide, sl] = -dot(nbuf[...], part, 1, 0)
        linv[low : low + wide, low : low + wide] = nbuf[...]

    end = nch - 1
    prev = end * wide
    first = other

    def last_rows(h, side, tc):
        mine = pl.ds(pl.multiple_of(side * CH, CH), CH)
        for j in range(end):
            at = pl.ds(pl.multiple_of(j * wide + tc * CH, CH), CH)
            pan[mine, at] += cg[end, tc, :, j * CH : (j + 1) * CH]
        out = slice(h * CH, (h + 1) * CH)
        for n in range(end):
            seen = (n + 1) * wide
            lp[out, n * wide : seen] = dot(pan[mine, :seen], linv[n * wide : seen, :seen], 1, 1)
        blk = gall[side, end * CH :, end * CH :] + jnp.where(eye, lam_ref[0], 0.0)
        s0[h] = blk - dot(lp[out, :], lp[out, :], 1, 1)

    def last_factor(ssem, rsem):
        gather_plane(cg.at[end], ssem, rsem)
        last_rows(0, first, t)

        def block(h, carry):
            @pl.when(h == 1)
            def _():
                gather_rest(cg.at[end], ssem, rsem)
                last_rows(1, t, first)
                both = cg[end, first, :, end * CH :] + cg[end, t, :, end * CH :].T
                l10 = dot(both - dot(lp[CH:, :], lp[:CH, :], 1, 1), w0[0], 1, 1)
                s0[1] -= dot(l10, l10, 1, 1)
                s1[:, :CH] = l10

            chol_inverse(s0.at[h], w0.at[h], LAST_STEP)
            return carry

        lax.fori_loop(0, 2, block, 0)
        n00, n11 = w0[0], w0[1]
        nbuf[:CH, :CH] = n00
        nbuf[:CH, CH:] = jnp.zeros((CH, CH), F32)
        nbuf[CH:, :CH] = -dot(n11, dot(s1[:, :CH], n00, 1, 0), 1, 0)
        nbuf[CH:, CH:] = n11

    for k in range(nch):
        if k:
            prepare(k)
        cross(k)
        if k == 0:
            diag_reduce()
            gather_start(gall, gs_sem.at[nch], gr_sem.at[nch])
            mom_swap(t).start()
        cross_reduce(k)
        gather_start(cg.at[k], gs_sem.at[k], gr_sem.at[k])
        issue(ahead[k], ahead[k + 1])
        if k == end:
            last_factor(gs_sem.at[k], gr_sem.at[k])
            break
        gather_finish(cg.at[k], gs_sem.at[k], gr_sem.at[k])
        if k == 0:
            gather_finish(gall, gs_sem.at[nch], gr_sem.at[nch])
            mom_swap(other).wait_recv()
            mom_swap(t).wait_send()
            for tt in range(2):
                hrow = jnp.broadcast_to(jnp.sum(hall[tt], axis=0, keepdims=True), (8, cols))
                for j in range(nch):
                    p = (2 * j + tt) * CH
                    hpos[:, p : p + CH] = hrow[:, j * CH : (j + 1) * CH]
            prepare(0)
        factor(k)

    def to_row(col):
        n = col.shape[0] // CH
        return jnp.concatenate(
            [jnp.sum(jnp.where(eye, col[i * CH : (i + 1) * CH], 0.0), axis=0, keepdims=True) for i in range(n)], axis=1
        )

    def to_col(row):
        n = row.shape[1] // CH
        return jnp.concatenate(
            [jnp.sum(jnp.where(eye, row[:, i * CH : (i + 1) * CH], 0.0), axis=1, keepdims=True) for i in range(n)], axis=0
        )

    def down(mat, col):
        return jnp.sum(mat * col, axis=0, keepdims=True)

    seen = jnp.sum(lp[...] * ybuf[0:1, :], axis=1, keepdims=True)
    tail = [hpos[0:1, prev : prev + CH], hpos[0:1, prev + CH :]]
    tail = jnp.concatenate([jnp.where(t == 1, tail[0], tail[1]), jnp.where(t == 1, tail[1], tail[0])], axis=1)
    rhs = tail - to_row(seen)
    ycol = jnp.sum(nbuf[...] * rhs, axis=1, keepdims=True)
    last = down(nbuf[...], ycol)
    ucol = to_col(ybuf[0:1, :] - down(lp[...], to_col(last)))
    rest = [down(linv[n * wide :, n * wide : (n + 1) * wide], ucol[n * wide :]) for n in range(nch - 1)]
    turn = [jnp.where(t == 1, last[:, :CH], last[:, CH:]), jnp.where(t == 1, last[:, CH:], last[:, :CH])]
    xpos = jnp.concatenate(rest + turn, axis=1)
    sides = [
        jnp.concatenate([xpos[0:1, (2 * j + tt) * CH : (2 * j + tt + 1) * CH] for j in range(nch)], axis=1) for tt in range(2)
    ]
    for tt in range(2):
        for j in range(nch):
            x_ref[tt * nch + j : tt * nch + j + 1, :] = sides[tt][:, j * CH : (j + 1) * CH]
    own = jnp.where(t == 0, sides[0], sides[1])
    x_swap = remote(x_ref, x_two.at[0], xx_sem.at[0], xx_sem.at[1], other, d)
    x_swap.start()

    def fit(m, carry):
        for g in range(8):
            blk = a_v[pl.ds(pl.multiple_of((m * 8 + g) * CH, CH), CH), :] * own
            tot = blk[:, :CH]
            for j in range(1, nch):
                tot = tot + blk[:, j * CH : (j + 1) * CH]
            tot = jnp.sum(tot, axis=1, keepdims=True)
            pbuf[pl.ds(m * 8 + g, 1), :] = jnp.sum(jnp.where(eye, tot, 0.0), axis=0, keepdims=True)
        return carry

    ngroup = rows // CH
    parts = ps_sem.shape[0]
    per = ngroup // parts

    def swap(q):
        sl = pl.ds(q * per, per)
        return remote(pbuf.at[sl, :], prec.at[sl, :], ps_sem.at[q], pr_sem.at[q], other, d)

    for q in range(parts):
        lax.fori_loop(q * per // 8, (q + 1) * per // 8, fit, 0)
        swap(q).start()
    x_swap.wait_recv()
    x_hbm[...] = jnp.where(t == 0, x_two[0], x_ref[...])
    for q in range(parts):
        swap(q).wait_recv()
        sl = pl.ds(q * per, per)
        r_hbm[sl, :] = b_ref[sl, :] - (pbuf[sl, :] + prec[sl, :])
    for q in range(parts):
        swap(q).wait_send()
    for q in range(total):
        exchange(q).wait_send()
    x_swap.wait_send()


def solution(mesh):
    def local_fit(design, target, ridge):
        rows, cols = design.shape
        half = rows // 2
        nch = cols // CH
        subs = 8
        nload = 16
        wide = 2 * CH
        prev = (nch - 1) * wide
        ngroup = rows // CH
        vm = pltpu.VMEM
        dma = pltpu.SemaphoreType.DMA
        scratch = [
            pltpu.SMEM((1,), F32),
            vm((ngroup, CH), F32),
            vm((2 * nch, CH), F32),
            vm((2, 2 * nch, CH), F32),
            vm((ngroup, CH), F32),
            vm((rows, cols), F32),
            vm((SLOTS, half, CH), F32),
            vm((cols, cols), F32),
            vm((8, cols), F32),
            vm((GROUPS - 1, cols // GROUPS, cols), F32),
            vm((GROUPS, 8, cols), F32),
            vm((2, cols, cols), F32),
            vm((2, 8, cols), F32),
            vm((CH, cols), F32),
            vm((nch, GROUPS - 1, CH // GROUPS, cols), F32),
            vm((nch, 2, CH, cols), F32),
            vm((wide, nch * wide), F32),
            vm((wide, prev), F32),
            vm((prev, prev), F32),
            vm((2, CH, CH), F32),
            vm((CH, wide), F32),
            vm((2, CH, CH), F32),
            vm((wide, wide), F32),
            vm((8, nch * wide), F32),
            vm((8, prev), F32),
            vm((ngroup, CH), F32),
            vm((ngroup, CH), F32),
            dma((3,)),
            dma((nload,)),
            dma((nch, subs)),
            dma((nch, subs)),
            dma((7,)),
            dma((7,)),
            dma((8,)),
            dma((8,)),
            dma((nch + 1, 15)),
            dma((nch + 1, 15)),
            dma((nch, 7)),
            dma((nch, 7)),
            dma((4,)),
            dma((4,)),
            dma((4,)),
            dma((2,)),
        ]
        x, r = pl.pallas_call(
            kernel,
            out_shape=(pltpu.VMEM((2 * nch, CH), F32), pltpu.VMEM((ngroup, CH), F32)),
            in_specs=[pl.BlockSpec(memory_space=pl.ANY)] * 3,
            out_specs=(pl.BlockSpec(memory_space=pltpu.VMEM), pl.BlockSpec(memory_space=pltpu.VMEM)),
            scratch_shapes=scratch,
            compiler_params=pltpu.CompilerParams(collective_id=0, has_side_effects=True, vmem_limit_bytes=66781184),
        )(ridge.reshape(1), target.reshape(ngroup, CH), design)
        return x.reshape(-1), r.reshape(-1)

    return jax.shard_map(
        local_fit, mesh=mesh, in_specs=(P("dp", "tp"), P("dp"), P()), out_specs=(P(), P("dp")), check_vma=False
    )
```
